32 devices in a mesh: dp: 2 (over core), sx: 4 (over y, x), sy: 4 (over z).
Axes of the slice: x: 2, y: 2, z: 4, core: 2. Of those that a mesh axis runs over, the one named last changes fastest.
Arguments:
- volume: bfloat16 [2, 32, 32, 32, 128], P('dp', None, 'sx', 'sy'), may hold values from -6 to 6
- conv_one: bfloat16 [2, 32, 32, 32, 128], P('dp', None, 'sx', 'sy'), may hold values from -300 to 300
- conv_two: bfloat16 [2, 32, 32, 32, 128], P('dp', None, 'sx', 'sy'), may hold values from -300 to 300
- upper_grad: bfloat16 [2, 32, 32, 32, 128], P('dp', None, 'sx', 'sy'), may hold values from -36 to 36
- weight_one: bfloat16 [3, 3, 3, 32, 32], replicated, may hold values from -0.21875 to 0.21875
- weight_two: bfloat16 [3, 3, 3, 32, 32], replicated, may hold values from -0.21875 to 0.21875
- gain_one: float32 [32], replicated, may hold values from 0.1 to 1.9
- bias_one: float32 [32], replicated, may hold values from -1 to 1
- gain_two: float32 [32], replicated, may hold values from 0.1 to 1.9
- bias_two: float32 [32], replicated, may hold values from -1 to 1
Outputs:
- input_grad: bfloat16 [2, 32, 32, 32, 128], P('dp', None, 'sx', 'sy')
- weight_one_grad: float32 [3, 3, 3, 32, 32], replicated
- weight_two_grad: float32 [3, 3, 3, 32, 32], replicated
- gain_one_grad: float32 [32], replicated
- bias_one_grad: float32 [32], replicated
- gain_two_grad: float32 [32], replicated
- bias_two_grad: float32 [32], replicated
The draws below stay inside these ranges and needn't reach their ends.
All inputs are finite; a program needn't handle non-finite values.
Results may differ from the reference program's by a relative error of at most 0.014.
Values may be sent and summed in bfloat16 or wider, within the bound.
A program may use at most 64 MiB of HBM per device.

```python
import math
import jax
import jax.numpy as jnp
from jax import lax

C = 32
CZ = 128
VOLS = 2
NX = 32
NY = 32


def rising_scale():
    volumes = jnp.arange(VOLS, dtype=jnp.float32) / max(VOLS - 1, 1)
    across = jnp.arange(NX, dtype=jnp.float32) / max(NX - 1, 1)
    along = jnp.arange(NY, dtype=jnp.float32) / max(NY - 1, 1)
    exponent = volumes[:, None, None, None, None] + across[None, None, :, None, None] + along[None, None, None, :, None] - 1.5
    return jnp.exp(exponent * math.log(3.0))


def saved_field(key):
    first, second, third = jax.random.split(key, 3)
    shape = (VOLS, C, NX, NY, CZ)
    offset = jax.random.uniform(first, (1, C, 1, 1, 1), jnp.float32, -1.0, 1.0)
    noise = jax.random.truncated_normal(second, -4.0, 4.0, shape, jnp.float32)
    factor = jnp.exp(jax.random.uniform(third, (VOLS, 1, NX, NY, CZ), jnp.float32, 0.0, math.log(10.0)))
    values = (offset + noise) * factor
    return (values * rising_scale()).astype(jnp.bfloat16)


def draw_conv_one(key, part):
    return saved_field(jax.random.fold_in(key, 11))


def draw_conv_two(key, part):
    return saved_field(jax.random.fold_in(key, 12))


def draw_upper_grad(key, part):
    first = jax.random.fold_in(jax.random.fold_in(key, 13), 0)
    shape = (VOLS, C, NX, NY, CZ)
    values = jax.random.truncated_normal(first, -4.0, 4.0, shape, jnp.float32)
    return (values * rising_scale()).astype(jnp.bfloat16)


def steps_of(own_key, extent, cuts, low, high):
    level = 1.0
    for axis_at, parts in cuts:
        steps = jax.random.uniform(jax.random.fold_in(jax.random.fold_in(own_key, 6), axis_at), (parts,), jnp.float32, low / len(cuts), high / len(cuts))
        level = level * jnp.repeat(jnp.exp(steps), extent[axis_at] // parts).reshape((-1,) + (1,) * (len(extent) - 1 - axis_at))
    return level


def scatter_about(stream_key, dims, deviation, bound, cuts=(), kind=jnp.bfloat16):
    array = jax.random.normal(stream_key, dims, jnp.float32) * deviation
    if len(cuts) > 0:
        array = steps_of(stream_key, dims, cuts, -0.22, 0.18) * array
    return jnp.clip(array, min=-bound, max=bound).astype(kind)


def setup_inputs(seed: int = 0) -> dict:
    key_of = jax.random.split(jax.random.key(seed), 11)
    volume = scatter_about(key_of[0], (VOLS, C, NX, NY, CZ), 1.0, 6.0, ((0, 2), (2, 4), (3, 4)))
    conv_one = draw_conv_one(jax.random.fold_in(key_of[10], 71), 0)
    conv_two = draw_conv_two(jax.random.fold_in(key_of[10], 71), 0)
    upper_grad = draw_upper_grad(jax.random.fold_in(key_of[10], 71), 0)
    weight_one = scatter_about(key_of[4], (3, 3, 3, C, C), (27 * C) ** -0.5, 0.21875)
    weight_two = scatter_about(key_of[5], (3, 3, 3, C, C), (27 * C) ** -0.5, 0.21875)
    gain_one = jnp.clip(1.0 + 0.18 * jax.random.normal(key_of[6], (C,), jnp.float32), 0.1, 1.9)
    bias_one = jnp.clip(jax.random.uniform(key_of[7], (C,), jnp.float32, -1.0, 1.0), -1.0, 1.0)
    gain_two = jnp.clip(1.0 + 0.18 * jax.random.normal(key_of[8], (C,), jnp.float32), 0.1, 1.9)
    bias_two = jnp.clip(jax.random.uniform(key_of[9], (C,), jnp.float32, -1.0, 1.0), -1.0, 1.0)
    return {"volume": volume, "conv_one": conv_one, "conv_two": conv_two, "upper_grad": upper_grad, "weight_one": weight_one, "weight_two": weight_two, "gain_one": gain_one, "bias_one": bias_one, "gain_two": gain_two, "bias_two": bias_two}


epsilon = 1e-05

def channel(vector):
    return vector[None, :, None, None, None]

def pad_space(values):
    return jnp.pad(values.astype(jnp.float32), ((0, 0), (0, 0), (1, 1), (1, 1), (1, 1)))

def back_project(gradient, weight):
    padded = pad_space(gradient)
    extent_x, extent_y, extent_z = (gradient.shape[2], gradient.shape[3], gradient.shape[4])
    total = jnp.zeros(gradient.shape, jnp.float32)
    for shift_x in range(3):
        for shift_y in range(3):
            for shift_z in range(3):
                piece = padded[:, :, 2 - shift_x:2 - shift_x + extent_x, 2 - shift_y:2 - shift_y + extent_y, 2 - shift_z:2 - shift_z + extent_z]
                total = total + jnp.einsum('co,boxyz->bcxyz', weight[shift_x, shift_y, shift_z].astype(jnp.float32), piece, precision=lax.Precision.HIGHEST)
    return total

def filter_terms(values, gradient):
    padded = pad_space(values)
    grad_full = gradient.astype(jnp.float32)
    extent_x, extent_y, extent_z = (gradient.shape[2], gradient.shape[3], gradient.shape[4])
    blocks = []
    for shift_x in range(3):
        for shift_y in range(3):
            for shift_z in range(3):
                piece = padded[:, :, shift_x:shift_x + extent_x, shift_y:shift_y + extent_y, shift_z:shift_z + extent_z]
                blocks.append(jnp.einsum('bcxyz,boxyz->co', piece, grad_full, precision=lax.Precision.HIGHEST))
    width = values.shape[1]
    return jnp.stack(blocks).reshape(3, 3, 3, width, gradient.shape[1])

def silu_slope(inputs):
    logistic = jax.nn.sigmoid(inputs)
    return logistic * (1.0 + inputs * (1.0 - logistic))

def normalized(saved, gain, offset, cell_count):
    saved_full = saved.astype(jnp.float32)
    total = lax.optimization_barrier(jnp.sum(saved_full, axis=(0, 2, 3, 4)))
    squares = lax.optimization_barrier(jnp.sum(saved_full * saved_full, axis=(0, 2, 3, 4)))
    average = total / cell_count
    spread = squares / cell_count - average * average
    inv_std = lax.rsqrt(spread + epsilon)
    centered = (saved_full - channel(average)) * channel(inv_std)
    shifted = channel(gain) * centered + channel(offset)
    return (centered, shifted, inv_std)

def norm_backward(upstream, centered, shifted, inv_std, gain, cell_count):
    slope_grad = upstream * silu_slope(shifted)
    bias_total = lax.optimization_barrier(jnp.sum(slope_grad, axis=(0, 2, 3, 4)))
    gain_total = lax.optimization_barrier(jnp.sum(slope_grad * centered, axis=(0, 2, 3, 4)))
    pre_grad = channel(gain * inv_std) * (slope_grad - channel(bias_total / cell_count) - centered * channel(gain_total / cell_count))
    return (pre_grad.astype(jnp.bfloat16), gain_total, bias_total)

def reference(volume, conv_one, conv_two, upper_grad, weight_one, weight_two, gain_one, bias_one, gain_two, bias_two):
    cell_count = float(VOLS * NX * NY * CZ)
    cent_one, shift_one, inv_one = normalized(conv_one, gain_one, bias_one, cell_count)
    activation = jax.nn.silu(shift_one).astype(jnp.bfloat16)
    cent_two, shift_two, inv_two = normalized(conv_two, gain_two, bias_two, cell_count)
    grad_two, gain_two_total, bias_two_total = norm_backward(upper_grad.astype(jnp.float32), cent_two, shift_two, inv_two, gain_two, cell_count)
    upstream = back_project(grad_two, weight_two)
    filter_two = filter_terms(activation, grad_two)
    grad_one, gain_one_total, bias_one_total = norm_backward(upstream, cent_one, shift_one, inv_one, gain_one, cell_count)
    input_grad = back_project(grad_one, weight_one).astype(jnp.bfloat16)
    filter_one = filter_terms(volume, grad_one)
    factor = 1.0 / math.sqrt(cell_count)
    return (input_grad, filter_one * factor, filter_two * factor, gain_one_total * factor, bias_one_total * factor, gain_two_total * factor, bias_two_total * factor)
```

```python
import functools
import math

import jax
import jax.numpy as jnp
from jax import lax
from jax.experimental import pallas as pl
from jax.experimental.pallas import tpu as pltpu
from jax.sharding import PartitionSpec as P

epsilon = 1e-05
AXES = ("dp", "sx", "sy")
NT = (((1,), (1,)), ((), ()))
F32 = jnp.float32
BF16 = jnp.bfloat16


def body(sizes, cells, c1, c2, ug, vol, w1, w2, g1, b1, g2, b2,
         out, filt, small,
         n1, n2, sl, d1, act, volp, grad, facc, ar, rb, og,
         ar_send, ar_recv, h_send, h_recv, rs_send, rs_recv, ag_send, ag_recv):
    n_dp, n_sx, n_sy = sizes
    n = n_dp * n_sx * n_sy
    ch, nx, ny, nz = c1.shape
    rows = ny * ch
    tiles = facc.shape[1]
    per = rb.shape[2]
    owners = tiles // per
    i_dp, i_sx, i_sy = [lax.axis_index(a) for a in AXES]
    me = (i_dp * n_sx + i_sx) * n_sy + i_sy

    def device(j):
        return (j // (n_sx * n_sy), (j // n_sy) % n_sx, j % n_sy)

    barrier = pltpu.get_barrier_semaphore()

    @pl.loop(1, n)
    def _(i):
        pl.semaphore_signal(barrier, inc=1, device_id=device((me + i) % n),
                            device_id_type=pl.DeviceIdType.MESH)

    r_i = lax.broadcasted_iota(jnp.int32, (rows, rows), 0)
    c_i = lax.broadcasted_iota(jnp.int32, (rows, rows), 1)
    perm = (c_i == (r_i % ch) * ny + r_i // ch).astype(F32).astype(BF16)
    back = (r_i == (c_i % ch) * ny + c_i // ch).astype(F32).astype(BF16)
    lane = lax.broadcasted_iota(jnp.int32, (ch, 128), 1)
    sub = lax.broadcasted_iota(jnp.int32, (ch, 128), 0)

    def load(ref, x):
        v = ref[:, x].astype(F32).reshape(rows, nz).astype(BF16)
        return jnp.dot(perm, v, preferred_element_type=F32)

    def per_channel(v):
        return jnp.sum(v.reshape(ny, ch, nz), axis=0)

    def tall(col):
        return jnp.concatenate([jnp.broadcast_to(col, (ch, nz))] * ny, axis=0)

    def column(row, q):
        wide = jnp.broadcast_to(row, (ch, 128))
        return jnp.sum(jnp.where(lane == sub + q * ch, wide, 0.0), axis=1, keepdims=True)

    def param(ref):
        wide = jnp.broadcast_to(ref[...], (ch, ch))
        return jnp.sum(jnp.where(lane[:, :ch] == sub[:, :ch], wide, 0.0), axis=1, keepdims=True)

    def start_sum(r, parts):
        parts = list(parts) + [jnp.zeros((ch, nz), F32)] * (128 // ch - len(parts))
        row = lax.dot_general(jnp.ones((8, nz), F32), jnp.concatenate(parts, axis=0), NT,
                              precision=lax.Precision.HIGHEST, preferred_element_type=F32)
        ar[r, me] = row[0:1]

        @pl.loop(1, n)
        def _(i):
            pltpu.make_async_remote_copy(
                ar.at[r, me], ar.at[r, me], ar_send.at[r], ar_recv.at[r],
                device_id=device((me + i) % n), device_id_type=pl.DeviceIdType.MESH).start()

    def end_sum(r):
        span = ar.at[r, pl.ds(0, n - 1)]
        pltpu.make_async_copy(span, span, ar_recv.at[r]).wait()
        pltpu.make_async_copy(span, span, ar_send.at[r]).wait()
        return jnp.sum(ar[r], axis=0)

    dirs = [(a, b) for a in (-1, 0, 1) for b in (-1, 0, 1) if (a, b) != (0, 0)]

    def side(step, extent, sending):
        if step == 0:
            return pl.ds(1, extent)
        if sending:
            return pl.ds(extent if step > 0 else 1, 1)
        return pl.ds(0 if step > 0 else extent + 1, 1)

    def halo_copy(k, d):
        a, b = dirs[d]
        return pltpu.make_async_remote_copy(
            grad.at[k, side(a, nx, True), side(b, ny, True), 1],
            grad.at[k, side(a, nx, False), side(b, ny, False), 1],
            h_send.at[k, d], h_recv.at[k, d],
            device_id=(i_dp, jnp.clip(i_sx + a, 0, n_sx - 1), jnp.clip(i_sy + b, 0, n_sy - 1)),
            device_id_type=pl.DeviceIdType.MESH)

    def there(a, b):
        return ((i_sx + a >= 0) & (i_sx + a < n_sx) & (i_sy + b >= 0) & (i_sy + b < n_sy))

    def start_halo(k):
        for d, (a, b) in enumerate(dirs):
            @pl.when(there(a, b))
            def _():
                halo_copy(k, d).start()

    lane_z = lax.broadcasted_iota(jnp.int32, (rows, nz), 1)

    def shifted(v):
        m = lane_z[: v.shape[0]]
        left = jnp.where(m == 0, 0.0, pltpu.roll(v, 1, 1))
        right = jnp.where(m == nz - 1, 0.0, pltpu.roll(v, nz - 1, 1))
        return left.astype(BF16), right.astype(BF16)

    def end_halo(k):
        for d, (a, b) in enumerate(dirs):
            @pl.when(there(-a, -b))
            def _():
                halo_copy(k, d).wait_recv()

            @pl.when(there(a, b))
            def _():
                halo_copy(k, d).wait_send()

        @pl.loop(0, ny)
        def _(i):
            for at in ((0, i + 1), (nx + 1, i + 1)):
                left, right = shifted(grad[k, at[0], at[1], 1].astype(F32))
                grad[k, at[0], at[1], 0] = left
                grad[k, at[0], at[1], 2] = right

        @pl.loop(0, nx + 2)
        def _(i):
            for at in (0, ny + 1):
                left, right = shifted(grad[k, i, at, 1].astype(F32))
                grad[k, i, at, 0] = left
                grad[k, i, at, 2] = right

    def project(w, k, x):
        pieces = []
        for y in range(ny):
            g = jnp.concatenate(
                [grad[k, x + a, y : y + 3].reshape(9 * ch, nz) for a in range(3)], axis=0)
            pieces.append(jnp.dot(w[...], g, preferred_element_type=F32))
        return jnp.concatenate(pieces, axis=0)

    def filters(k, u):
        facc[k] = jnp.zeros(facc.shape[1:], F32)

        @pl.loop(0, nx + 2)
        def _(x):
            lhs = jnp.concatenate(
                [grad[k, x, y : y + 3].reshape(9 * ch, nz) for y in range(ny)], axis=1)
            rhs = jnp.concatenate(
                [u[y, pl.ds(x, 3)].reshape(3 * ch, nz) for y in range(ny)], axis=1)
            rhs = jnp.concatenate([rhs, jnp.zeros((128 - 3 * ch, ny * nz), BF16)], axis=0)
            r = lax.dot_general(lhs, rhs, NT, preferred_element_type=F32)
            facc[k] += r.reshape(facc.shape[1:])

    def start_scatter(k):
        @pl.loop(0, owners)
        def _(i):
            j = (me + i) % owners

            @pl.when(j != me)
            def _():
                pltpu.make_async_remote_copy(
                    facc.at[k, pl.ds(j * per, per)], rb.at[k, me], rs_send.at[k], rs_recv.at[k],
                    device_id=device(j), device_id_type=pl.DeviceIdType.MESH).start()

    def wait_bytes(ref, sem):
        pltpu.make_async_copy(ref, ref, sem).wait()

    def start_gather(k):
        @pl.when(me < owners)
        def _():
            mine = pl.ds(me * per, per)
            rb[k, me] = facc[k, mine]
            wait_bytes(rb.at[k, pl.ds(0, n - 1)], rs_recv.at[k])
            og[k, mine] = jnp.sum(rb[k], axis=0) * (1.0 / math.sqrt(cells))

            @pl.loop(1, n)
            def _(i):
                pltpu.make_async_remote_copy(
                    og.at[k, mine], og.at[k, mine], ag_send.at[k], ag_recv.at[k],
                    device_id=device((me + i) % n), device_id_type=pl.DeviceIdType.MESH).start()

    def end_gather(k):
        @pl.when(me < owners)
        def _():
            wait_bytes(facc.at[k, pl.ds(0, (owners - 1) * per)], rs_send.at[k])
            wait_bytes(og.at[k, pl.ds(0, (owners - 1) * per)], ag_recv.at[k])
            wait_bytes(rb.at[k, pl.ds(0, n - 1)], ag_send.at[k])

        @pl.when(me >= owners)
        def _():
            wait_bytes(facc.at[k], rs_send.at[k])
            wait_bytes(og.at[k], ag_recv.at[k])

        filt[k] = og[k]

    zero = jnp.zeros((ch, nz), F32)

    def moments(x, acc):
        v1, v2 = load(c1, x), load(c2, x)
        n1[x], n2[x] = v1, v2
        sl[x] = load(ug, x)
        new = (v1, v1 * v1, v2, v2 * v2)
        return tuple(a + per_channel(v) for a, v in zip(acc, new))

    parts = lax.fori_loop(0, nx, moments, (zero,) * 4)
    for k in range(2):
        grad[k, pl.ds(0, 1)] = jnp.zeros((1,) + grad.shape[2:], BF16)
        grad[k, pl.ds(nx + 1, 1)] = jnp.zeros((1,) + grad.shape[2:], BF16)
        for at in (0, ny + 1):
            grad[k, :, at] = jnp.zeros((nx + 2,) + grad.shape[3:], BF16)
    pl.semaphore_wait(barrier, n - 1)
    start_sum(0, parts)

    for u in (act, volp):
        for at in (0, nx + 2):
            u[:, pl.ds(at, 2)] = jnp.zeros((ny, 2, ch, nz), BF16)

    @pl.loop(0, nx)
    def _(x):
        volp[:, x + 2] = load(vol, x).astype(BF16).reshape(ny, ch, nz)

    total = end_sum(0)

    def norm(q):
        mean = column(total, q) / cells
        spread = column(total, q + 1) / cells - mean * mean
        return mean, lax.rsqrt(spread + epsilon)

    mean1, inv1 = norm(0)
    mean2, inv2 = norm(2)
    gain1, bias1, gain2, bias2 = param(g1), param(b1), param(g2), param(b2)
    mean1_t, inv1_t, gain1_t, bias1_t = tall(mean1), tall(inv1), tall(gain1), tall(bias1)
    mean2_t, inv2_t, gain2_t, bias2_t = tall(mean2), tall(inv2), tall(gain2), tall(bias2)

    def slope_two(x, acc):
        cent = (n2[x] - mean2_t) * inv2_t
        v = gain2_t * cent + bias2_t
        s = jax.nn.sigmoid(v)
        slope = sl[x] * (s * (1.0 + v * (1.0 - s)))
        n2[x] = cent
        sl[x] = slope
        return acc[0] + per_channel(slope), acc[1] + per_channel(slope * cent)

    start_sum(1, lax.fori_loop(0, nx, slope_two, (zero, zero)))

    @pl.loop(0, nx)
    def _(x):
        cent = (n1[x] - mean1_t) * inv1_t
        v = gain1_t * cent + bias1_t
        s = jax.nn.sigmoid(v)
        n1[x] = cent
        d1[x] = s * (1.0 + v * (1.0 - s))
        act[:, x + 2] = (v * s).astype(BF16).reshape(ny, ch, nz)

    def make_grad(k, row, cent, scale):
        bsum, gsum = tall(column(row, 0) / cells), tall(column(row, 1) / cells)
        scale = tall(scale)

        @pl.loop(0, nx)
        def _(x):
            v = scale * (sl[x] - bsum - cent[x] * gsum)
            left, right = shifted(v)
            for kz, part in enumerate((left, v.astype(BF16), right)):
                grad[k, x + 1, pl.ds(1, ny), kz] = part.reshape(ny, ch, nz)

    factor = 1.0 / math.sqrt(cells)
    row = end_sum(1)
    small[0:1] = row * factor
    make_grad(0, row, n2, gain2 * inv2)
    start_halo(0)
    end_halo(0)

    def slope_one(x, acc):
        slope = project(w2, 0, x) * d1[x]
        sl[x] = slope
        return acc[0] + per_channel(slope), acc[1] + per_channel(slope * n1[x])

    start_sum(2, lax.fori_loop(0, nx, slope_one, (zero, zero)))
    filters(0, act)
    start_scatter(0)
    row = end_sum(2)
    small[1:2] = row * factor
    make_grad(1, row, n1, gain1 * inv1)
    start_halo(1)
    start_gather(0)
    end_halo(1)
    filters(1, volp)
    start_scatter(1)

    @pl.loop(0, nx)
    def _(x):
        v = project(w1, 1, x).astype(BF16)
        out[:, x] = jnp.dot(back, v, preferred_element_type=F32).reshape(ch, ny, nz).astype(BF16)

    start_gather(1)
    end_gather(0)
    end_gather(1)


def per_device(volume, conv_one, conv_two, upper_grad, weight_one, weight_two,
               gain_one, bias_one, gain_two, bias_two):
    sizes = tuple(lax.axis_size(a) for a in AXES)
    n = math.prod(sizes)
    _, ch, nx, ny, nz = volume.shape
    cells = float(volume.shape[0] * nx * ny * nz * n)
    tiles = 9 * ch // 8
    per = -(-tiles // n)
    while tiles % per:
        per += 1

    def flat(w):
        return jnp.transpose(w[::-1, ::-1, ::-1], (3, 0, 1, 2, 4)).reshape(ch, 27 * ch)

    vmem = pl.BlockSpec(memory_space=pltpu.VMEM)
    dma = pltpu.SemaphoreType.DMA
    big = pltpu.VMEM((nx, ny * ch, nz), F32)
    pad_u = pltpu.VMEM((ny, nx + 4, ch, nz), BF16)
    out, filt, small = pl.pallas_call(
        functools.partial(body, sizes, cells),
        name="section_backward",
        out_shape=(
            jax.ShapeDtypeStruct((ch, nx, ny, nz), BF16),
            jax.ShapeDtypeStruct((2, tiles, 8, 128), F32),
            jax.ShapeDtypeStruct((8, 128), F32),
        ),
        in_specs=[vmem] * 10,
        out_specs=(vmem,) * 3,
        scratch_shapes=[
            big, big, big, big, pad_u, pad_u,
            pltpu.VMEM((2, nx + 2, ny + 2, 3, ch, nz), BF16),
            pltpu.VMEM((2, tiles, 8, 128), F32),
            pltpu.VMEM((3, n, 1, 128), F32),
            pltpu.VMEM((2, n, per, 8, 128), F32),
            pltpu.VMEM((2, tiles, 8, 128), F32),
            dma((3,)), dma((3,)), dma((2, 8)), dma((2, 8)),
            dma((2,)), dma((2,)), dma((2,)), dma((2,)),
        ],
        compiler_params=pltpu.CompilerParams(
            collective_id=0, has_side_effects=True, vmem_limit_bytes=60 * 1024 * 1024),
    )(conv_one[0], conv_two[0], upper_grad[0], volume[0], flat(weight_one), flat(weight_two),
      gain_one[None], bias_one[None], gain_two[None], bias_two[None])

    def unflat(f):
        f = f.reshape(3, 3, ch, 128)[..., : 3 * ch].reshape(3, 3, ch, 3, ch)
        return jnp.transpose(f, (3, 0, 1, 4, 2))[:, ::-1, ::-1]

    return (out[None], unflat(filt[1]), unflat(filt[0]),
            small[1, ch : 2 * ch], small[1, :ch], small[0, ch : 2 * ch], small[0, :ch])


def solution(mesh):
    block = P("dp", None, "sx", "sy", None)
    return jax.shard_map(
        per_device,
        mesh=mesh,
        in_specs=(block,) * 4 + (P(),) * 6,
        out_specs=(block,) + (P(),) * 6,
        check_vma=False,
    )
```

```python
import functools
import math

import jax
import jax.numpy as jnp
from jax import lax
from jax.experimental import pallas as pl
from jax.experimental.pallas import tpu as pltpu
from jax.sharding import PartitionSpec as P

epsilon = 1e-05
AXES = ("dp", "sx", "sy")
NT = (((1,), (1,)), ((), ()))
F32 = jnp.float32
BF16 = jnp.bfloat16


def body(sizes, cells, c1, c2, ug, vol, w1, w2, g1, b1, g2, b2,
         out, og, small,
         n1, n2, sl, d1, act, volp, grad, facc, ar, rb, wt, hx, hc, hs,
         ar_send, ar_recv, h_send, h_recv, rs_send, rs_recv, ag_send, ag_recv):
    n_dp, n_sx, n_sy = sizes
    n = n_dp * n_sx * n_sy
    ch, nx, ny, nz = c1.shape
    rows = ny * ch
    tiles = facc.shape[1]
    per = rb.shape[2]
    owners = tiles // per
    i_dp, i_sx, i_sy = [lax.axis_index(a) for a in AXES]
    me = (i_dp * n_sx + i_sx) * n_sy + i_sy

    def each_peer(use):
        def step(_, at):
            a, b, c = at
            c = c + 1
            b = jnp.where(c == n_sy, b + 1, b)
            c = jnp.where(c == n_sy, 0, c)
            a = jnp.where(b == n_sx, a + 1, a)
            b = jnp.where(b == n_sx, 0, b)
            a = jnp.where(a == n_dp, 0, a)
            use((a, b, c))
            return a, b, c

        lax.fori_loop(0, n - 1, step, (i_dp, i_sx, i_sy))

    barrier = pltpu.get_barrier_semaphore()

    @each_peer
    def _(peer):
        pl.semaphore_signal(barrier, inc=1, device_id=peer,
                            device_id_type=pl.DeviceIdType.MESH)

    r_i = lax.broadcasted_iota(jnp.int32, (rows, rows), 0)
    c_i = lax.broadcasted_iota(jnp.int32, (rows, rows), 1)
    perm = (c_i == (r_i % ch) * ny + r_i // ch).astype(F32).astype(BF16)
    lane = lax.broadcasted_iota(jnp.int32, (ch, 128), 1)
    sub = lax.broadcasted_iota(jnp.int32, (ch, 128), 0)

    def load(ref, x):
        v = ref[:, x].astype(F32).reshape(rows, nz).astype(BF16)
        return jnp.dot(perm, v, preferred_element_type=F32)

    def per_channel(v):
        return jnp.sum(v.reshape(ny, ch, nz), axis=0)

    def tall(col):
        return jnp.concatenate([jnp.broadcast_to(col, (ch, nz))] * ny, axis=0)

    def column(row, q):
        wide = jnp.broadcast_to(row, (ch, 128))
        return jnp.sum(jnp.where(lane == sub + q * ch, wide, 0.0), axis=1, keepdims=True)

    def param(ref):
        wide = jnp.broadcast_to(ref[...], (ch, ch))
        return jnp.sum(jnp.where(lane[:, :ch] == sub[:, :ch], wide, 0.0), axis=1, keepdims=True)

    def start_sum(r, parts):
        parts = list(parts) + [jnp.zeros((ch, nz), F32)] * (128 // ch - len(parts))
        row = lax.dot_general(jnp.ones((8, nz), F32), jnp.concatenate(parts, axis=0), NT,
                              precision=lax.Precision.HIGHEST, preferred_element_type=F32)
        ar[r, me] = row[0:1]

        @each_peer
        def _(peer):
            pltpu.make_async_remote_copy(
                ar.at[r, me], ar.at[r, me], ar_send.at[r], ar_recv.at[r],
                device_id=peer, device_id_type=pl.DeviceIdType.MESH).start()

    def end_sum(r):
        span = ar.at[r, pl.ds(0, n - 1)]
        pltpu.make_async_copy(span, span, ar_recv.at[r]).wait()
        pltpu.make_async_copy(span, span, ar_send.at[r]).wait()
        return jnp.sum(ar[r], axis=0)

    dirs = [(a, b) for a in (-1, 0, 1) for b in (-1, 0, 1) if (a, b) != (0, 0)]

    def side(step, extent, sending):
        if step == 0:
            return pl.ds(1, extent)
        if sending:
            return pl.ds(extent if step > 0 else 1, 1)
        return pl.ds(0 if step > 0 else extent + 1, 1)

    def halo_copy(k, d):
        a, b = dirs[d]
        return pltpu.make_async_remote_copy(
            hx.at[k, side(a, nx, True), side(b, ny, True)],
            hx.at[k, side(a, nx, False), side(b, ny, False)],
            h_send.at[k, d], h_recv.at[k, d],
            device_id=(i_dp, jnp.clip(i_sx + a, 0, n_sx - 1), jnp.clip(i_sy + b, 0, n_sy - 1)),
            device_id_type=pl.DeviceIdType.MESH)

    def there(a, b):
        return ((i_sx + a >= 0) & (i_sx + a < n_sx) & (i_sy + b >= 0) & (i_sy + b < n_sy))

    def start_halo(k):
        for d, (a, b) in enumerate(dirs):
            @pl.when(there(a, b))
            def _():
                halo_copy(k, d).start()

    lane_z = lax.broadcasted_iota(jnp.int32, (rows + 2 * ch, nz), 1)

    def shifted(v):
        m = lane_z[: v.shape[0]]
        left = jnp.where(m == 0, 0.0, pltpu.roll(v, 1, 1))
        right = jnp.where(m == nz - 1, 0.0, pltpu.roll(v, nz - 1, 1))
        return left.astype(BF16), right.astype(BF16)

    def end_halo(k):
        for d, (a, b) in enumerate(dirs):
            @pl.when(there(-a, -b))
            def _():
                halo_copy(k, d).wait_recv()

            @pl.when(there(a, b))
            def _():
                halo_copy(k, d).wait_send()

    rims = [(0, None, ny + 2), (nx + 1, None, ny + 2), (None, 0, nx), (None, ny + 1, nx)]

    def rim_of(q, i):
        x, y, m = rims[i]
        return (hx[q, x] if y is None else hx[q, pl.ds(1, nx), y]).astype(F32)

    def inside(i):
        x, y, m = rims[i]
        at = lax.broadcasted_iota(jnp.int32, (m, ch, nz), 0)
        if y is None:
            fixed, size, low, limit = i_sx * nx + x - 1, n_sx * nx, i_sy * ny - 1, n_sy * ny
        else:
            fixed, size, low, limit = i_sy * ny + y - 1, n_sy * ny, 0, nx + 1
        bound = jnp.where((fixed >= 0) & (fixed < size), 0, limit)
        return (at + low >= bound) & (at + low < limit)

    def rim_grad(k, bsum, gsum, scale):
        for i, (x, y, m) in enumerate(rims):
            slope = hs[i, pl.ds(0, m)] if k == 0 else rim_of(3, i)
            v = scale * (slope - bsum - hc[k, i, pl.ds(0, m)] * gsum)
            v = jnp.where(inside(i), v, 0.0).reshape(m * ch, nz)
            left, right = shifted(v)
            for kz, part in enumerate((left, v.astype(BF16), right)):
                part = part.reshape(m, ch, nz)
                if y is None:
                    grad[k, x, :, kz] = part
                else:
                    grad[k, pl.ds(1, nx), y, kz] = part

    def project(k, x):
        w = wt[k, :, pl.ds(0, 27 * ch)]
        pieces = []
        for y in range(ny):
            g = jnp.concatenate(
                [grad[k, x + a, y : y + 3].reshape(9 * ch, nz) for a in range(3)], axis=0)
            pieces.append(jnp.dot(w, g, preferred_element_type=F32))
        return jnp.concatenate(pieces, axis=0)

    def filters(k, u):
        facc[k] = jnp.zeros(facc.shape[1:], F32)

        @pl.loop(0, nx + 2)
        def _(x):
            lhs = jnp.concatenate(
                [grad[k, x, y : y + 3].reshape(9 * ch, nz) for y in range(ny)], axis=1)
            rhs = jnp.concatenate(
                [u[y, pl.ds(x, 3)].reshape(3 * ch, nz) for y in range(ny)], axis=1)
            rhs = jnp.concatenate([rhs, jnp.zeros((128 - 3 * ch, ny * nz), BF16)], axis=0)
            r = lax.dot_general(lhs, rhs, NT, preferred_element_type=F32)
            facc[k] += r.reshape(facc.shape[1:])

    def start_scatter(k):
        @each_peer
        def _(peer):
            j = (peer[0] * n_sx + peer[1]) * n_sy + peer[2]

            @pl.when(j < owners)
            def _():
                pltpu.make_async_remote_copy(
                    facc.at[k, pl.ds(j * per, per)], rb.at[k, me], rs_send.at[k], rs_recv.at[k],
                    device_id=peer, device_id_type=pl.DeviceIdType.MESH).start()

    def wait_bytes(ref, sem):
        pltpu.make_async_copy(ref, ref, sem).wait()

    def start_gather(k):
        @pl.when(me < owners)
        def _():
            mine = pl.ds(me * per, per)
            rb[k, me] = facc[k, mine]
            wait_bytes(rb.at[k, pl.ds(0, n - 1)], rs_recv.at[k])
            og[k, mine] = jnp.sum(rb[k], axis=0) * (1.0 / math.sqrt(cells))

            @each_peer
            def _(peer):
                pltpu.make_async_remote_copy(
                    og.at[k, mine], og.at[k, mine], ag_send.at[k], ag_recv.at[k],
                    device_id=peer, device_id_type=pl.DeviceIdType.MESH).start()

    def end_gather(k):
        @pl.when(me < owners)
        def _():
            wait_bytes(facc.at[k, pl.ds(0, (owners - 1) * per)], rs_send.at[k])
            wait_bytes(og.at[k, pl.ds(0, (owners - 1) * per)], ag_recv.at[k])
            wait_bytes(rb.at[k, pl.ds(0, n - 1)], ag_send.at[k])

        @pl.when(me >= owners)
        def _():
            wait_bytes(facc.at[k], rs_send.at[k])
            wait_bytes(og.at[k], ag_recv.at[k])

    zero = jnp.zeros((ch, nz), F32)

    def moments(x, acc):
        v1, v2 = load(c1, x), load(c2, x)
        n1[x], n2[x] = v1, v2
        v3 = load(ug, x)
        sl[x] = v3
        for q, v in enumerate((v2, v3, v1)):
            hx[q, x + 1, pl.ds(1, ny)] = v.astype(BF16).reshape(ny, ch, nz)
        new = (v1, v1 * v1, v2, v2 * v2)
        return tuple(a + per_channel(v) for a, v in zip(acc, new))

    parts = lax.fori_loop(0, nx, moments, (zero,) * 4)
    pl.semaphore_wait(barrier, n - 1)
    start_sum(0, parts)
    start_halo(0)
    start_halo(1)

    group = 128 // ch
    for k, w in enumerate((w2, w1)):
        for first in range(0, 27, group):
            total = jnp.zeros((ch, 128), F32)
            for t in range(first, min(first + group, 27)):
                r = 26 - t
                pick = (lane == sub + (t - first) * ch).astype(F32).astype(BF16)
                total += jnp.dot(w[r // 9, r // 3 % 3, r % 3], pick, preferred_element_type=F32)
            wt[k, :, pl.ds(first * ch, 128)] = total.astype(BF16)

    for u in (act, volp):
        for at in (0, nx + 2):
            u[:, pl.ds(at, 2)] = jnp.zeros((ny, 2, ch, nz), BF16)

    @pl.loop(0, nx)
    def _(x):
        volp[:, x + 2] = load(vol, x).astype(BF16).reshape(ny, ch, nz)

    total = end_sum(0)

    def norm(q):
        mean = column(total, q) / cells
        spread = column(total, q + 1) / cells - mean * mean
        return mean, lax.rsqrt(spread + epsilon)

    mean1, inv1 = norm(0)
    mean2, inv2 = norm(2)
    gain1, bias1, gain2, bias2 = param(g1), param(b1), param(g2), param(b2)
    mean1_t, inv1_t, gain1_t, bias1_t = tall(mean1), tall(inv1), tall(gain1), tall(bias1)
    mean2_t, inv2_t, gain2_t, bias2_t = tall(mean2), tall(inv2), tall(gain2), tall(bias2)

    def slope_two(x, acc):
        cent = (n2[x] - mean2_t) * inv2_t
        v = gain2_t * cent + bias2_t
        s = jax.nn.sigmoid(v)
        slope = sl[x] * (s * (1.0 + v * (1.0 - s)))
        n2[x] = cent
        sl[x] = slope
        return acc[0] + per_channel(slope), acc[1] + per_channel(slope * cent)

    start_sum(1, lax.fori_loop(0, nx, slope_two, (zero, zero)))
    start_halo(2)

    @pl.loop(0, nx)
    def _(x):
        cent = (n1[x] - mean1_t) * inv1_t
        v = gain1_t * cent + bias1_t
        s = jax.nn.sigmoid(v)
        n1[x] = cent
        d1[x] = s * (1.0 + v * (1.0 - s))
        act[:, x + 2] = (v * s).astype(BF16).reshape(ny, ch, nz)

    def make_grad(k, row, cent, scale):
        bsum, gsum = column(row, 0) / cells, column(row, 1) / cells
        rim_grad(k, wide(bsum), wide(gsum), wide(scale))
        bsum, gsum, scale = tall(bsum), tall(gsum), tall(scale)

        @pl.loop(0, nx)
        def _(x):
            v = scale * (sl[x] - bsum - cent[x] * gsum)
            left, right = shifted(v)
            for kz, part in enumerate((left, v.astype(BF16), right)):
                grad[k, x + 1, pl.ds(1, ny), kz] = part.reshape(ny, ch, nz)

    def wide(col):
        return jnp.broadcast_to(col, (ch, nz))[None]

    end_halo(0)
    end_halo(1)
    for i in range(4):
        m = rims[i][2]
        cent = (rim_of(0, i) - wide(mean2)) * wide(inv2)
        v = wide(gain2) * cent + wide(bias2)
        s = jax.nn.sigmoid(v)
        hc[0, i, pl.ds(0, m)] = cent
        hs[i, pl.ds(0, m)] = rim_of(1, i) * (s * (1.0 + v * (1.0 - s)))

    factor = 1.0 / math.sqrt(cells)
    row = end_sum(1)
    small[0:1] = row * factor
    make_grad(0, row, n2, gain2 * inv2)

    def slope_one(x, acc):
        slope = project(0, x) * d1[x]
        sl[x] = slope
        hx[3, x + 1, pl.ds(1, ny)] = slope.astype(BF16).reshape(ny, ch, nz)
        return acc[0] + per_channel(slope), acc[1] + per_channel(slope * n1[x])

    start_sum(2, lax.fori_loop(0, nx, slope_one, (zero, zero)))
    start_halo(3)
    filters(0, act)
    start_scatter(0)
    end_halo(2)
    for i in range(4):
        hc[1, i, pl.ds(0, rims[i][2])] = (rim_of(2, i) - wide(mean1)) * wide(inv1)
    row = end_sum(2)
    small[1:2] = row * factor
    end_halo(3)
    make_grad(1, row, n1, gain1 * inv1)
    start_gather(0)
    filters(1, volp)
    start_scatter(1)

    @pl.loop(0, nx)
    def _(x):
        out[x] = project(1, x).astype(BF16)

    start_gather(1)
    end_gather(0)
    end_gather(1)


def finish(rows_in, og, small, out, f1, f2, g1, b1, g2, b2):
    ch, nx, ny, nz = out.shape
    rows = ny * ch
    r_i = lax.broadcasted_iota(jnp.int32, (rows, rows), 0)
    c_i = lax.broadcasted_iota(jnp.int32, (rows, rows), 1)
    back = (r_i == (c_i % ch) * ny + c_i // ch).astype(F32).astype(BF16)
    for x in range(nx):
        v = jnp.dot(back, rows_in[x], preferred_element_type=F32)
        out[:, x] = v.reshape(ch, ny, nz).astype(BF16)
    for k, f in enumerate((f2, f1)):
        for b in range(9):
            t = og[k, pl.ds(b * ch // 8, ch // 8)].reshape(ch, 128).T
            for kx in range(3):
                f[kx, 2 - b // 3, 2 - b % 3] = t[kx * ch : (kx + 1) * ch]
    for r, (b, g) in enumerate(((b2, g2), (b1, g1))):
        b[...] = small[r : r + 1, :ch]
        g[...] = small[r : r + 1, ch : 2 * ch]


def per_device(volume, conv_one, conv_two, upper_grad, weight_one, weight_two,
               gain_one, bias_one, gain_two, bias_two):
    sizes = tuple(lax.axis_size(a) for a in AXES)
    n = math.prod(sizes)
    _, ch, nx, ny, nz = volume.shape
    cells = float(volume.shape[0] * nx * ny * nz * n)
    tiles = 9 * ch // 8
    per = -(-tiles // n)
    while tiles % per:
        per += 1

    vmem = pl.BlockSpec(memory_space=pltpu.VMEM)
    dma = pltpu.SemaphoreType.DMA
    big = pltpu.VMEM((nx, ny * ch, nz), F32)
    pad_u = pltpu.VMEM((ny, nx + 4, ch, nz), BF16)
    mid = pl.pallas_call(
        functools.partial(body, sizes, cells),
        name="section_backward",
        out_shape=(
            jax.ShapeDtypeStruct((nx, ny * ch, nz), BF16),
            jax.ShapeDtypeStruct((2, tiles, 8, 128), F32),
            jax.ShapeDtypeStruct((8, 128), F32),
        ),
        in_specs=[vmem] * 10,
        out_specs=(vmem,) * 3,
        scratch_shapes=[
            big, big, big, big, pad_u, pad_u,
            pltpu.VMEM((2, nx + 2, ny + 2, 3, ch, nz), BF16),
            pltpu.VMEM((2, tiles, 8, 128), F32),
            pltpu.VMEM((3, n, 1, 128), F32),
            pltpu.VMEM((2, n, per, 8, 128), F32),
            pltpu.VMEM((2, ch, -(-27 * ch // 128) * 128), BF16),
            pltpu.VMEM((4, nx + 2, ny + 2, ch, nz), BF16),
            pltpu.VMEM((2, 4, max(nx, ny) + 2, ch, nz), F32),
            pltpu.VMEM((4, max(nx, ny) + 2, ch, nz), F32),
            dma((3,)), dma((3,)), dma((4, 8)), dma((4, 8)),
            dma((2,)), dma((2,)), dma((2,)), dma((2,)),
        ],
        compiler_params=pltpu.CompilerParams(
            collective_id=0, has_side_effects=True, vmem_limit_bytes=60 * 1024 * 1024),
    )(conv_one[0], conv_two[0], upper_grad[0], volume[0], weight_one, weight_two,
      gain_one[None], bias_one[None], gain_two[None], bias_two[None])

    vector = jax.ShapeDtypeStruct((1, ch), F32)
    filt = jax.ShapeDtypeStruct(weight_one.shape, F32)
    out, *rest = pl.pallas_call(
        finish,
        name="section_finish",
        out_shape=(jax.ShapeDtypeStruct((ch, nx, ny, nz), BF16), filt, filt) + (vector,) * 4,
        in_specs=[vmem] * 3,
        out_specs=(vmem,) * 7,
    )(*mid)
    return (out[None], *rest[:2], *(v[0] for v in rest[2:]))


def solution(mesh):
    block = P("dp", None, "sx", "sy", None)
    return jax.shard_map(
        per_device,
        mesh=mesh,
        in_specs=(block,) * 4 + (P(),) * 6,
        out_specs=(block,) + (P(),) * 6,
        check_vma=False,
    )
```

```python
import functools
import math

import jax
import jax.numpy as jnp
from jax import lax
from jax.experimental import pallas as pl
from jax.experimental.pallas import tpu as pltpu
from jax.sharding import PartitionSpec as P

epsilon = 1e-05
AXES = ("dp", "sx", "sy")
NT = (((1,), (1,)), ((), ()))
F32 = jnp.float32
BF16 = jnp.bfloat16


def body(sizes, cells, c1, c2, ug, vol, w1, w2, g1, b1, g2, b2,
         out, og, small,
         n1, n2, sl, d1, act, volp, grad, facc, fb, ar, rb, wt, hx, hc, hs,
         ar_send, ar_recv, h_send, h_recv, rs_send, rs_recv, ag_send, ag_recv):
    n_dp, n_sx, n_sy = sizes
    n = n_dp * n_sx * n_sy
    ch, nx, ny, nz = c1.shape
    rows = ny * ch
    tiles = fb.shape[1]
    per = rb.shape[2]
    owners = tiles // per
    i_dp, i_sx, i_sy = [lax.axis_index(a) for a in AXES]
    me = (i_dp * n_sx + i_sx) * n_sy + i_sy

    def each_peer(use):
        def step(_, at):
            a, b, c = at
            c = c + 1
            b = jnp.where(c == n_sy, b + 1, b)
            c = jnp.where(c == n_sy, 0, c)
            a = jnp.where(b == n_sx, a + 1, a)
            b = jnp.where(b == n_sx, 0, b)
            a = jnp.where(a == n_dp, 0, a)
            use((a, b, c))
            return a, b, c

        lax.fori_loop(0, n - 1, step, (i_dp, i_sx, i_sy))

    barrier = pltpu.get_barrier_semaphore()

    @each_peer
    def _(peer):
        pl.semaphore_signal(barrier, inc=1, device_id=peer,
                            device_id_type=pl.DeviceIdType.MESH)

    r_i = lax.broadcasted_iota(jnp.int32, (rows, rows), 0)
    c_i = lax.broadcasted_iota(jnp.int32, (rows, rows), 1)
    perm = (c_i == (r_i % ch) * ny + r_i // ch).astype(F32).astype(BF16)
    lane = lax.broadcasted_iota(jnp.int32, (ch, 128), 1)
    sub = lax.broadcasted_iota(jnp.int32, (ch, 128), 0)

    def load(ref, x):
        v = ref[:, x].astype(F32).reshape(rows, nz).astype(BF16)
        return jnp.dot(perm, v, preferred_element_type=F32)

    def per_channel(v):
        return jnp.sum(v.reshape(ny, ch, nz), axis=0)

    def tall(col):
        return jnp.concatenate([jnp.broadcast_to(col, (ch, nz))] * ny, axis=0)

    def column(row, q):
        wide = jnp.broadcast_to(row, (ch, 128))
        return jnp.sum(jnp.where(lane == sub + q * ch, wide, 0.0), axis=1, keepdims=True)

    def param(ref):
        wide = jnp.broadcast_to(ref[...], (ch, ch))
        return jnp.sum(jnp.where(lane[:, :ch] == sub[:, :ch], wide, 0.0), axis=1, keepdims=True)

    def start_sum(r, parts):
        parts = list(parts) + [jnp.zeros((ch, nz), F32)] * (128 // ch - len(parts))
        row = lax.dot_general(jnp.ones((8, nz), F32), jnp.concatenate(parts, axis=0), NT,
                              precision=lax.Precision.HIGHEST, preferred_element_type=F32)
        ar[r, me] = row[0:1]

        @each_peer
        def _(peer):
            pltpu.make_async_remote_copy(
                ar.at[r, me], ar.at[r, me], ar_send.at[r], ar_recv.at[r],
                device_id=peer, device_id_type=pl.DeviceIdType.MESH).start()

    def end_sum(r):
        span = ar.at[r, pl.ds(0, n - 1)]
        pltpu.make_async_copy(span, span, ar_recv.at[r]).wait()
        pltpu.make_async_copy(span, span, ar_send.at[r]).wait()
        return jnp.sum(ar[r], axis=0)

    dirs = [(a, b) for a in (-1, 0, 1) for b in (-1, 0, 1) if (a, b) != (0, 0)]

    def side(step, extent, sending):
        if step == 0:
            return pl.ds(1, extent)
        if sending:
            return pl.ds(extent if step > 0 else 1, 1)
        return pl.ds(0 if step > 0 else extent + 1, 1)

    def halo_copy(k, d):
        a, b = dirs[d]
        return pltpu.make_async_remote_copy(
            hx.at[k, side(a, nx, True), side(b, ny, True)],
            hx.at[k, side(a, nx, False), side(b, ny, False)],
            h_send.at[k, d], h_recv.at[k, d],
            device_id=(i_dp, jnp.clip(i_sx + a, 0, n_sx - 1), jnp.clip(i_sy + b, 0, n_sy - 1)),
            device_id_type=pl.DeviceIdType.MESH)

    def there(a, b):
        return ((i_sx + a >= 0) & (i_sx + a < n_sx) & (i_sy + b >= 0) & (i_sy + b < n_sy))

    def start_halo(k):
        for d, (a, b) in enumerate(dirs):
            @pl.when(there(a, b))
            def _():
                halo_copy(k, d).start()

    lane_z = lax.broadcasted_iota(jnp.int32, (rows + 2 * ch, nz), 1)

    def shifted(v):
        m = lane_z[: v.shape[0]]
        left = jnp.where(m == 0, 0.0, pltpu.roll(v, 1, 1))
        right = jnp.where(m == nz - 1, 0.0, pltpu.roll(v, nz - 1, 1))
        return left.astype(BF16), right.astype(BF16)

    def end_halo(k):
        for d, (a, b) in enumerate(dirs):
            @pl.when(there(-a, -b))
            def _():
                halo_copy(k, d).wait_recv()

            @pl.when(there(a, b))
            def _():
                halo_copy(k, d).wait_send()

    rims = [(0, None, ny + 2), (nx + 1, None, ny + 2), (None, 0, nx), (None, ny + 1, nx)]

    def rim_of(q, i):
        x, y, m = rims[i]
        return (hx[q, x] if y is None else hx[q, pl.ds(1, nx), y]).astype(F32)

    def inside(i):
        x, y, m = rims[i]
        at = lax.broadcasted_iota(jnp.int32, (m, ch, nz), 0)
        if y is None:
            fixed, size, low, limit = i_sx * nx + x - 1, n_sx * nx, i_sy * ny - 1, n_sy * ny
        else:
            fixed, size, low, limit = i_sy * ny + y - 1, n_sy * ny, 0, nx + 1
        bound = jnp.where((fixed >= 0) & (fixed < size), 0, limit)
        return (at + low >= bound) & (at + low < limit)

    def rim_grad(k, bsum, gsum, scale):
        for i, (x, y, m) in enumerate(rims):
            slope = hs[i, pl.ds(0, m)] if k == 0 else rim_of(3, i)
            v = scale * (slope - bsum - hc[k, i, pl.ds(0, m)] * gsum)
            v = jnp.where(inside(i), v, 0.0).reshape(m * ch, nz)
            left, right = shifted(v)
            for kz, part in enumerate((left, v.astype(BF16), right)):
                part = part.reshape(m, ch, nz)
                if y is None:
                    grad[k, x, :, kz] = part
                else:
                    grad[k, pl.ds(1, nx), y, kz] = part

    def project(k, x):
        w = wt[k, :, pl.ds(0, 27 * ch)]
        pieces = []
        pair = 2 if ny % 2 == 0 else 1
        for first in range(0, ny, pair):
            g = jnp.concatenate([
                jnp.concatenate(
                    [grad[k, x + a, y : y + 3].reshape(9 * ch, nz) for a in range(3)], axis=0)
                for y in range(first, first + pair)], axis=1)
            r = jnp.dot(w, g, preferred_element_type=F32)
            pieces += [r[:, i * nz : (i + 1) * nz] for i in range(pair)]
        return jnp.concatenate(pieces, axis=0)

    def filters(k, u):
        facc[k] = jnp.zeros(facc.shape[1:], F32)
        pair = 2 if nx % 2 == 0 else 1

        @pl.loop(0, (nx + 2) // pair)
        def _(step):
            xs = [step * pair + i for i in range(pair)]
            lhs = jnp.concatenate(
                [grad[k, x, y : y + 3].reshape(9 * ch, nz) for x in xs for y in range(ny)], axis=1)
            rhs = jnp.concatenate(
                [u[y, pl.ds(x, 3)].reshape(3 * ch, nz) for x in xs for y in range(ny)], axis=1)
            rhs = jnp.concatenate(
                [rhs, jnp.zeros((128 - 3 * ch, rhs.shape[1]), BF16)], axis=0)
            facc[k] += lax.dot_general(lhs, rhs, NT, preferred_element_type=F32)

        fb[k] = facc[k].reshape(fb.shape[1:]).astype(BF16)

    def place(k, j):
        return j if k == 0 else n - 1 - j

    def start_scatter(k):
        @each_peer
        def _(peer):
            j = (peer[0] * n_sx + peer[1]) * n_sy + peer[2]

            @pl.when(place(k, j) < owners)
            def _():
                pltpu.make_async_remote_copy(
                    fb.at[k, pl.ds(place(k, j) * per, per)], rb.at[k, me], rs_send.at[k], rs_recv.at[k],
                    device_id=peer, device_id_type=pl.DeviceIdType.MESH).start()

    def wait_bytes(ref, sem):
        pltpu.make_async_copy(ref, ref, sem).wait()

    def start_gather(k):
        @pl.when(place(k, me) < owners)
        def _():
            mine = pl.ds(place(k, me) * per, per)
            rb[k, me] = fb[k, mine]
            wait_bytes(rb.at[k, pl.ds(0, n - 1)], rs_recv.at[k])
            og[k, mine] = (
                jnp.sum(rb[k].astype(F32), axis=0) * (1.0 / math.sqrt(cells))).astype(BF16)

            @each_peer
            def _(peer):
                pltpu.make_async_remote_copy(
                    og.at[k, mine], og.at[k, mine], ag_send.at[k], ag_recv.at[k],
                    device_id=peer, device_id_type=pl.DeviceIdType.MESH).start()

    def end_gather(k):
        @pl.when(place(k, me) < owners)
        def _():
            wait_bytes(fb.at[k, pl.ds(0, (owners - 1) * per)], rs_send.at[k])
            wait_bytes(og.at[k, pl.ds(0, (owners - 1) * per)], ag_recv.at[k])
            wait_bytes(rb.at[k, pl.ds(0, n - 1)], ag_send.at[k])

        @pl.when(place(k, me) >= owners)
        def _():
            wait_bytes(fb.at[k], rs_send.at[k])
            wait_bytes(og.at[k], ag_recv.at[k])

    zero = jnp.zeros((ch, nz), F32)

    def moments(x, acc):
        v1, v2 = load(c1, x), load(c2, x)
        n1[x], n2[x] = v1, v2
        v3 = load(ug, x)
        sl[x] = v3
        for q, v in enumerate((v2, v3, v1)):
            hx[q, x + 1, pl.ds(1, ny)] = v.astype(BF16).reshape(ny, ch, nz)
        new = (v1, v1 * v1, v2, v2 * v2)
        return tuple(a + per_channel(v) for a, v in zip(acc, new))

    parts = lax.fori_loop(0, nx, moments, (zero,) * 4)
    pl.semaphore_wait(barrier, n - 1)
    start_sum(0, parts)
    start_halo(0)
    start_halo(1)

    group = 128 // ch
    for k, w in enumerate((w2, w1)):
        for first in range(0, 27, group):
            total = jnp.zeros((ch, 128), F32)
            for t in range(first, min(first + group, 27)):
                r = 26 - t
                pick = (lane == sub + (t - first) * ch).astype(F32).astype(BF16)
                total += jnp.dot(w[r // 9, r // 3 % 3, r % 3], pick, preferred_element_type=F32)
            wt[k, :, pl.ds(first * ch, 128)] = total.astype(BF16)

    for u in (act, volp):
        for at in (0, nx + 2):
            u[:, pl.ds(at, 2)] = jnp.zeros((ny, 2, ch, nz), BF16)

    @pl.loop(0, nx)
    def _(x):
        volp[:, x + 2] = load(vol, x).astype(BF16).reshape(ny, ch, nz)

    total = end_sum(0)

    def norm(q):
        mean = column(total, q) / cells
        spread = column(total, q + 1) / cells - mean * mean
        return mean, lax.rsqrt(spread + epsilon)

    mean1, inv1 = norm(0)
    mean2, inv2 = norm(2)
    gain1, bias1, gain2, bias2 = param(g1), param(b1), param(g2), param(b2)
    mean1_t, inv1_t, gain1_t, bias1_t = tall(mean1), tall(inv1), tall(gain1), tall(bias1)
    mean2_t, inv2_t, gain2_t, bias2_t = tall(mean2), tall(inv2), tall(gain2), tall(bias2)

    def slope_two(x, acc):
        cent = (n2[x] - mean2_t) * inv2_t
        v = gain2_t * cent + bias2_t
        s = jax.nn.sigmoid(v)
        slope = sl[x] * (s * (1.0 + v * (1.0 - s)))
        n2[x] = cent
        sl[x] = slope
        return acc[0] + per_channel(slope), acc[1] + per_channel(slope * cent)

    start_sum(1, lax.fori_loop(0, nx, slope_two, (zero, zero)))
    start_halo(2)

    @pl.loop(0, nx)
    def _(x):
        cent = (n1[x] - mean1_t) * inv1_t
        v = gain1_t * cent + bias1_t
        s = jax.nn.sigmoid(v)
        n1[x] = cent
        d1[x] = s * (1.0 + v * (1.0 - s))
        act[:, x + 2] = (v * s).astype(BF16).reshape(ny, ch, nz)

    def make_grad(k, row, cent, scale):
        bsum, gsum = column(row, 0) / cells, column(row, 1) / cells
        rim_grad(k, wide(bsum), wide(gsum), wide(scale))
        bsum, gsum, scale = tall(bsum), tall(gsum), tall(scale)

        @pl.loop(0, nx)
        def _(x):
            v = scale * (sl[x] - bsum - cent[x] * gsum)
            left, right = shifted(v)
            for kz, part in enumerate((left, v.astype(BF16), right)):
                grad[k, x + 1, pl.ds(1, ny), kz] = part.reshape(ny, ch, nz)

    def wide(col):
        return jnp.broadcast_to(col, (ch, nz))[None]

    end_halo(0)
    end_halo(1)
    for i in range(4):
        m = rims[i][2]
        cent = (rim_of(0, i) - wide(mean2)) * wide(inv2)
        v = wide(gain2) * cent + wide(bias2)
        s = jax.nn.sigmoid(v)
        hc[0, i, pl.ds(0, m)] = cent
        hs[i, pl.ds(0, m)] = rim_of(1, i) * (s * (1.0 + v * (1.0 - s)))

    factor = 1.0 / math.sqrt(cells)
    row = end_sum(1)
    small[0:1] = row * factor
    make_grad(0, row, n2, gain2 * inv2)

    def slope_one(x, acc):
        slope = project(0, x) * d1[x]
        sl[x] = slope
        hx[3, x + 1, pl.ds(1, ny)] = slope.astype(BF16).reshape(ny, ch, nz)
        return acc[0] + per_channel(slope), acc[1] + per_channel(slope * n1[x])

    start_sum(2, lax.fori_loop(0, nx, slope_one, (zero, zero)))
    start_halo(3)
    filters(0, act)
    start_scatter(0)
    end_halo(2)
    for i in range(4):
        hc[1, i, pl.ds(0, rims[i][2])] = (rim_of(2, i) - wide(mean1)) * wide(inv1)
    row = end_sum(2)
    small[1:2] = row * factor
    end_halo(3)
    make_grad(1, row, n1, gain1 * inv1)
    filters(1, volp)
    start_scatter(1)
    start_gather(0)

    @pl.loop(0, nx)
    def _(x):
        out[x] = project(1, x).astype(BF16)

    start_gather(1)
    end_gather(0)
    end_gather(1)


def finish(rows_in, og, small, out, f1, f2, g1, b1, g2, b2):
    ch, nx, ny, nz = out.shape
    rows = ny * ch
    r_i = lax.broadcasted_iota(jnp.int32, (rows, rows), 0)
    c_i = lax.broadcasted_iota(jnp.int32, (rows, rows), 1)
    back = (r_i == (c_i % ch) * ny + c_i // ch).astype(F32).astype(BF16)
    for x in range(nx):
        v = jnp.dot(back, rows_in[x], preferred_element_type=F32)
        out[:, x] = v.reshape(ch, ny, nz).astype(BF16)
    for k, f in enumerate((f2, f1)):
        for b in range(9):
            t = og[k, pl.ds(b * ch // 16, ch // 16)].reshape(ch, 128).astype(F32).T
            for kx in range(3):
                f[kx, 2 - b // 3, 2 - b % 3] = t[kx * ch : (kx + 1) * ch]
    for r, (b, g) in enumerate(((b2, g2), (b1, g1))):
        b[...] = small[r : r + 1, :ch]
        g[...] = small[r : r + 1, ch : 2 * ch]


def per_device(volume, conv_one, conv_two, upper_grad, weight_one, weight_two,
               gain_one, bias_one, gain_two, bias_two):
    sizes = tuple(lax.axis_size(a) for a in AXES)
    n = math.prod(sizes)
    _, ch, nx, ny, nz = volume.shape
    cells = float(volume.shape[0] * nx * ny * nz * n)
    tiles = 9 * ch // 16
    per = -(-tiles // n)
    while tiles % per:
        per += 1

    vmem = pl.BlockSpec(memory_space=pltpu.VMEM)
    dma = pltpu.SemaphoreType.DMA
    big = pltpu.VMEM((nx, ny * ch, nz), F32)
    pad_u = pltpu.VMEM((ny, nx + 4, ch, nz), BF16)
    mid = pl.pallas_call(
        functools.partial(body, sizes, cells),
        name="section_backward",
        out_shape=(
            jax.ShapeDtypeStruct((nx, ny * ch, nz), BF16),
            jax.ShapeDtypeStruct((2, tiles, 16, 128), BF16),
            jax.ShapeDtypeStruct((8, 128), F32),
        ),
        in_specs=[vmem] * 10,
        out_specs=(vmem,) * 3,
        scratch_shapes=[
            big, big, big, big, pad_u, pad_u,
            pltpu.VMEM((2, nx + 2, ny + 2, 3, ch, nz), BF16),
            pltpu.VMEM((2, 9 * ch, 128), F32),
            pltpu.VMEM((2, tiles, 16, 128), BF16),
            pltpu.VMEM((3, n, 1, 128), F32),
            pltpu.VMEM((2, n, per, 16, 128), BF16),
            pltpu.VMEM((2, ch, -(-27 * ch // 128) * 128), BF16),
            pltpu.VMEM((4, nx + 2, ny + 2, ch, nz), BF16),
            pltpu.VMEM((2, 4, max(nx, ny) + 2, ch, nz), F32),
            pltpu.VMEM((4, max(nx, ny) + 2, ch, nz), F32),
            dma((3,)), dma((3,)), dma((4, 8)), dma((4, 8)),
            dma((2,)), dma((2,)), dma((2,)), dma((2,)),
        ],
        compiler_params=pltpu.CompilerParams(
            collective_id=0, has_side_effects=True, vmem_limit_bytes=60 * 1024 * 1024),
    )(conv_one[0], conv_two[0], upper_grad[0], volume[0], weight_one, weight_two,
      gain_one[None], bias_one[None], gain_two[None], bias_two[None])

    vector = jax.ShapeDtypeStruct((1, ch), F32)
    filt = jax.ShapeDtypeStruct(weight_one.shape, F32)
    out, *rest = pl.pallas_call(
        finish,
        name="section_finish",
        out_shape=(jax.ShapeDtypeStruct((ch, nx, ny, nz), BF16), filt, filt) + (vector,) * 4,
        in_specs=[vmem] * 3,
        out_specs=(vmem,) * 7,
    )(*mid)
    return (out[None], *rest[:2], *(v[0] for v in rest[2:]))


def solution(mesh):
    block = P("dp", None, "sx", "sy", None)
    return jax.shard_map(
        per_device,
        mesh=mesh,
        in_specs=(block,) * 4 + (P(),) * 6,
        out_specs=(block,) + (P(),) * 6,
        check_vma=False,
    )
```

```python
import functools
import math

import jax
import jax.numpy as jnp
from jax import lax
from jax.experimental import pallas as pl
from jax.experimental.pallas import tpu as pltpu
from jax.sharding import PartitionSpec as P

epsilon = 1e-05
AXES = ("dp", "sx", "sy")
NT = (((1,), (1,)), ((), ()))
F32 = jnp.float32
BF16 = jnp.bfloat16


def body(sizes, cells, c1, c2, ug, vol, w1, w2, g1, b1, g2, b2,
         out, og, small,
         n1, n2, sl, d1, act, volp, grad, facc, fb, ar, rb, wt, hx, hc, hs,
         ar_send, ar_recv, h_send, h_recv, rs_send, rs_recv, ag_send, ag_recv):
    n_dp, n_sx, n_sy = sizes
    n = n_dp * n_sx * n_sy
    ch, nx, ny, nz = c1.shape
    rows = ny * ch
    tiles = fb.shape[1]
    per = rb.shape[2]
    owners = tiles // per
    i_dp, i_sx, i_sy = [lax.axis_index(a) for a in AXES]
    me = (i_dp * n_sx + i_sx) * n_sy + i_sy

    def each_peer(use):
        def step(_, at):
            a, b, c = at
            c = c + 1
            b = jnp.where(c == n_sy, b + 1, b)
            c = jnp.where(c == n_sy, 0, c)
            a = jnp.where(b == n_sx, a + 1, a)
            b = jnp.where(b == n_sx, 0, b)
            a = jnp.where(a == n_dp, 0, a)
            use((a, b, c))
            return a, b, c

        lax.fori_loop(0, n - 1, step, (i_dp, i_sx, i_sy))

    barrier = pltpu.get_barrier_semaphore()

    @each_peer
    def _(peer):
        pl.semaphore_signal(barrier, inc=1, device_id=peer,
                            device_id_type=pl.DeviceIdType.MESH)

    r_i = lax.broadcasted_iota(jnp.int32, (rows, rows), 0)
    c_i = lax.broadcasted_iota(jnp.int32, (rows, rows), 1)
    perm = (c_i == (r_i % ch) * ny + r_i // ch).astype(F32).astype(BF16)
    lane = lax.broadcasted_iota(jnp.int32, (ch, 128), 1)
    sub = lax.broadcasted_iota(jnp.int32, (ch, 128), 0)

    def load(ref, x):
        v = ref[:, x].astype(F32).reshape(rows, nz).astype(BF16)
        return jnp.dot(perm, v, preferred_element_type=F32)

    def per_channel(v):
        return jnp.sum(v.reshape(ny, ch, nz), axis=0)

    def tall(col):
        return jnp.concatenate([jnp.broadcast_to(col, (ch, nz))] * ny, axis=0)

    def column(row, q):
        wide = jnp.broadcast_to(row, (ch, 128))
        return jnp.sum(jnp.where(lane == sub + q * ch, wide, 0.0), axis=1, keepdims=True)

    def param(ref):
        wide = jnp.broadcast_to(ref[...], (ch, ch))
        return jnp.sum(jnp.where(lane[:, :ch] == sub[:, :ch], wide, 0.0), axis=1, keepdims=True)

    def start_sum(r, parts):
        parts = list(parts) + [jnp.zeros((ch, nz), F32)] * (128 // ch - len(parts))
        row = lax.dot_general(jnp.ones((8, nz), F32), jnp.concatenate(parts, axis=0), NT,
                              precision=lax.Precision.HIGHEST, preferred_element_type=F32)
        ar[r, me] = row[0:1]

        @each_peer
        def _(peer):
            pltpu.make_async_remote_copy(
                ar.at[r, me], ar.at[r, me], ar_send.at[r], ar_recv.at[r],
                device_id=peer, device_id_type=pl.DeviceIdType.MESH).start()

    def end_sum(r):
        span = ar.at[r, pl.ds(0, n - 1)]
        pltpu.make_async_copy(span, span, ar_recv.at[r]).wait()
        pltpu.make_async_copy(span, span, ar_send.at[r]).wait()
        return jnp.sum(ar[r], axis=0)

    dirs = [(a, b) for a in (-1, 0, 1) for b in (-1, 0, 1) if (a, b) != (0, 0)]

    def side(step, extent, sending):
        if step == 0:
            return pl.ds(1, extent)
        if sending:
            return pl.ds(extent if step > 0 else 1, 1)
        return pl.ds(0 if step > 0 else extent + 1, 1)

    def halo_copy(k, d):
        a, b = dirs[d]
        return pltpu.make_async_remote_copy(
            hx.at[k, side(a, nx, True), side(b, ny, True)],
            hx.at[k, side(a, nx, False), side(b, ny, False)],
            h_send.at[k, d], h_recv.at[k, d],
            device_id=(i_dp, jnp.clip(i_sx + a, 0, n_sx - 1), jnp.clip(i_sy + b, 0, n_sy - 1)),
            device_id_type=pl.DeviceIdType.MESH)

    def there(a, b):
        return ((i_sx + a >= 0) & (i_sx + a < n_sx) & (i_sy + b >= 0) & (i_sy + b < n_sy))

    def start_halo(k):
        for d, (a, b) in enumerate(dirs):
            @pl.when(there(a, b))
            def _():
                halo_copy(k, d).start()

    lane_z = lax.broadcasted_iota(jnp.int32, (rows + 2 * ch, nz), 1)

    def shifted(v):
        m = lane_z[: v.shape[0]]
        left = jnp.where(m == 0, 0.0, pltpu.roll(v, 1, 1))
        right = jnp.where(m == nz - 1, 0.0, pltpu.roll(v, nz - 1, 1))
        return left.astype(BF16), right.astype(BF16)

    def end_halo(k):
        for d, (a, b) in enumerate(dirs):
            @pl.when(there(-a, -b))
            def _():
                halo_copy(k, d).wait_recv()

            @pl.when(there(a, b))
            def _():
                halo_copy(k, d).wait_send()

    rims = [(0, None, ny + 2), (nx + 1, None, ny + 2), (None, 0, nx), (None, ny + 1, nx)]

    def rim_of(q, i):
        x, y, m = rims[i]
        return (hx[q, x] if y is None else hx[q, pl.ds(1, nx), y]).astype(F32)

    def inside(i):
        x, y, m = rims[i]
        at = lax.broadcasted_iota(jnp.int32, (m, ch, nz), 0)
        if y is None:
            fixed, size, low, limit = i_sx * nx + x - 1, n_sx * nx, i_sy * ny - 1, n_sy * ny
        else:
            fixed, size, low, limit = i_sy * ny + y - 1, n_sy * ny, 0, nx + 1
        bound = jnp.where((fixed >= 0) & (fixed < size), 0, limit)
        return (at + low >= bound) & (at + low < limit)

    def rim_grad(k, bsum, gsum, scale):
        for i, (x, y, m) in enumerate(rims):
            slope = hs[i, pl.ds(0, m)] if k == 0 else rim_of(3, i)
            v = scale * (slope - bsum - hc[k, i, pl.ds(0, m)] * gsum)
            v = jnp.where(inside(i), v, 0.0).reshape(m * ch, nz)
            left, right = shifted(v)
            for kz, part in enumerate((left, v.astype(BF16), right)):
                part = part.reshape(m, ch, nz)
                if y is None:
                    grad[k, x, :, kz] = part
                else:
                    grad[k, pl.ds(1, nx), y, kz] = part

    def project(k, x):
        w = wt[k, :, pl.ds(0, 27 * ch)]
        pieces = []
        pair = 2 if ny % 2 == 0 else 1
        for first in range(0, ny, pair):
            g = jnp.concatenate([
                jnp.concatenate(
                    [grad[k, x + a, y : y + 3].reshape(9 * ch, nz) for a in range(3)], axis=0)
                for y in range(first, first + pair)], axis=1)
            r = jnp.dot(w, g, preferred_element_type=F32)
            pieces += [r[:, i * nz : (i + 1) * nz] for i in range(pair)]
        return jnp.concatenate(pieces, axis=0)

    def filters(k, u):
        facc[k] = jnp.zeros(facc.shape[1:], F32)
        pair = 2 if nx % 2 == 0 else 1

        @pl.loop(0, (nx + 2) // pair)
        def _(step):
            xs = [step * pair + i for i in range(pair)]
            lhs = jnp.concatenate(
                [grad[k, x, y : y + 3].reshape(9 * ch, nz) for x in xs for y in range(ny)], axis=1)
            rhs = jnp.concatenate(
                [u[y, pl.ds(x, 3)].reshape(3 * ch, nz) for x in xs for y in range(ny)], axis=1)
            rhs = jnp.concatenate(
                [rhs, jnp.zeros((128 - 3 * ch, rhs.shape[1]), BF16)], axis=0)
            facc[k] += lax.dot_general(lhs, rhs, NT, preferred_element_type=F32)

        fb[k] = facc[k].reshape(fb.shape[1:]).astype(BF16)

    def place(k, j):
        return j if k == 0 else n - 1 - j

    def start_scatter(k):
        @each_peer
        def _(peer):
            j = (peer[0] * n_sx + peer[1]) * n_sy + peer[2]

            @pl.when(place(k, j) < owners)
            def _():
                pltpu.make_async_remote_copy(
                    fb.at[k, pl.ds(place(k, j) * per, per)], rb.at[k, me], rs_send.at[k], rs_recv.at[k],
                    device_id=peer, device_id_type=pl.DeviceIdType.MESH).start()

    def wait_bytes(ref, sem):
        pltpu.make_async_copy(ref, ref, sem).wait()

    def start_gather(k):
        @pl.when(place(k, me) < owners)
        def _():
            mine = pl.ds(place(k, me) * per, per)
            rb[k, me] = fb[k, mine]
            wait_bytes(rb.at[k, pl.ds(0, n - 1)], rs_recv.at[k])
            og[k, mine] = (
                jnp.sum(rb[k].astype(F32), axis=0) * (1.0 / math.sqrt(cells))).astype(BF16)

            @each_peer
            def _(peer):
                pltpu.make_async_remote_copy(
                    og.at[k, mine], og.at[k, mine], ag_send.at[k], ag_recv.at[k],
                    device_id=peer, device_id_type=pl.DeviceIdType.MESH).start()

    def end_gather(k):
        @pl.when(place(k, me) < owners)
        def _():
            wait_bytes(fb.at[k, pl.ds(0, (owners - 1) * per)], rs_send.at[k])
            wait_bytes(og.at[k, pl.ds(0, (owners - 1) * per)], ag_recv.at[k])
            wait_bytes(rb.at[k, pl.ds(0, n - 1)], ag_send.at[k])

        @pl.when(place(k, me) >= owners)
        def _():
            wait_bytes(fb.at[k], rs_send.at[k])
            wait_bytes(og.at[k], ag_recv.at[k])

    zero = jnp.zeros((ch, nz), F32)

    def moments(x, acc):
        v1, v2 = load(c1, x), load(c2, x)
        n1[x], n2[x] = v1, v2
        v3 = load(ug, x)
        sl[x] = v3
        for q, v in enumerate((v2, v3, v1)):
            hx[q, x + 1, pl.ds(1, ny)] = v.astype(BF16).reshape(ny, ch, nz)
        new = (v1, v1 * v1, v2, v2 * v2)
        return tuple(a + per_channel(v) for a, v in zip(acc, new))

    parts = lax.fori_loop(0, nx, moments, (zero,) * 4, unroll=True)
    pl.semaphore_wait(barrier, n - 1)
    start_sum(0, parts)
    start_halo(0)
    start_halo(1)

    group = 128 // ch
    for k, w in enumerate((w2, w1)):
        for first in range(0, 27, group):
            total = jnp.zeros((ch, 128), F32)
            for t in range(first, min(first + group, 27)):
                r = 26 - t
                pick = (lane == sub + (t - first) * ch).astype(F32).astype(BF16)
                total += jnp.dot(w[r // 9, r // 3 % 3, r % 3], pick, preferred_element_type=F32)
            wt[k, :, pl.ds(first * ch, 128)] = total.astype(BF16)

    for u in (act, volp):
        for at in (0, nx + 2):
            u[:, pl.ds(at, 2)] = jnp.zeros((ny, 2, ch, nz), BF16)

    @pl.loop(0, nx, unroll=True)
    def _(x):
        volp[:, x + 2] = load(vol, x).astype(BF16).reshape(ny, ch, nz)

    total = end_sum(0)

    def norm(q):
        mean = column(total, q) / cells
        spread = column(total, q + 1) / cells - mean * mean
        return mean, lax.rsqrt(spread + epsilon)

    mean1, inv1 = norm(0)
    mean2, inv2 = norm(2)
    gain1, bias1, gain2, bias2 = param(g1), param(b1), param(g2), param(b2)
    mean1_t, inv1_t, gain1_t, bias1_t = tall(mean1), tall(inv1), tall(gain1), tall(bias1)
    mean2_t, inv2_t, gain2_t, bias2_t = tall(mean2), tall(inv2), tall(gain2), tall(bias2)

    def slope_two(x, acc):
        cent = (n2[x] - mean2_t) * inv2_t
        v = gain2_t * cent + bias2_t
        s = jax.nn.sigmoid(v)
        slope = sl[x] * (s * (1.0 + v * (1.0 - s)))
        n2[x] = cent
        sl[x] = slope
        return acc[0] + per_channel(slope), acc[1] + per_channel(slope * cent)

    start_sum(1, lax.fori_loop(0, nx, slope_two, (zero, zero)))
    start_halo(2)

    @pl.loop(0, nx)
    def _(x):
        cent = (n1[x] - mean1_t) * inv1_t
        v = gain1_t * cent + bias1_t
        s = jax.nn.sigmoid(v)
        n1[x] = cent
        d1[x] = s * (1.0 + v * (1.0 - s))
        act[:, x + 2] = (v * s).astype(BF16).reshape(ny, ch, nz)

    def make_grad(k, row, cent, scale):
        bsum, gsum = column(row, 0) / cells, column(row, 1) / cells
        rim_grad(k, wide(bsum), wide(gsum), wide(scale))
        bsum, gsum, scale = tall(bsum), tall(gsum), tall(scale)

        @pl.loop(0, nx)
        def _(x):
            v = scale * (sl[x] - bsum - cent[x] * gsum)
            left, right = shifted(v)
            for kz, part in enumerate((left, v.astype(BF16), right)):
                grad[k, x + 1, pl.ds(1, ny), kz] = part.reshape(ny, ch, nz)

    def wide(col):
        return jnp.broadcast_to(col, (ch, nz))[None]

    end_halo(0)
    end_halo(1)
    for i in range(4):
        m = rims[i][2]
        cent = (rim_of(0, i) - wide(mean2)) * wide(inv2)
        v = wide(gain2) * cent + wide(bias2)
        s = jax.nn.sigmoid(v)
        hc[0, i, pl.ds(0, m)] = cent
        hs[i, pl.ds(0, m)] = rim_of(1, i) * (s * (1.0 + v * (1.0 - s)))

    factor = 1.0 / math.sqrt(cells)
    row = end_sum(1)
    small[0:1] = row * factor
    make_grad(0, row, n2, gain2 * inv2)

    def slope_one(x, acc):
        slope = project(0, x) * d1[x]
        sl[x] = slope
        hx[3, x + 1, pl.ds(1, ny)] = slope.astype(BF16).reshape(ny, ch, nz)
        return acc[0] + per_channel(slope), acc[1] + per_channel(slope * n1[x])

    start_sum(2, lax.fori_loop(0, nx, slope_one, (zero, zero), unroll=True))
    start_halo(3)
    filters(0, act)
    start_scatter(0)
    end_halo(2)
    for i in range(4):
        hc[1, i, pl.ds(0, rims[i][2])] = (rim_of(2, i) - wide(mean1)) * wide(inv1)
    row = end_sum(2)
    small[1:2] = row * factor
    end_halo(3)
    make_grad(1, row, n1, gain1 * inv1)
    filters(1, volp)
    start_scatter(1)
    start_gather(0)

    split = nx - nx // 4

    @pl.loop(0, split, unroll=True)
    def _(x):
        out[x] = project(1, x).astype(BF16)

    start_gather(1)

    @pl.loop(split, nx, unroll=True)
    def _(x):
        out[x] = project(1, x).astype(BF16)

    end_gather(0)
    end_gather(1)


def finish(rows_in, og, small, out, f1, f2, g1, b1, g2, b2):
    ch, nx, ny, nz = out.shape
    rows = ny * ch
    r_i = lax.broadcasted_iota(jnp.int32, (rows, rows), 0)
    c_i = lax.broadcasted_iota(jnp.int32, (rows, rows), 1)
    back = (r_i == (c_i % ch) * ny + c_i // ch).astype(F32).astype(BF16)
    for x in range(nx):
        v = jnp.dot(back, rows_in[x], preferred_element_type=F32)
        out[:, x] = v.reshape(ch, ny, nz).astype(BF16)
    for k, f in enumerate((f2, f1)):
        for b in range(9):
            t = og[k, pl.ds(b * ch // 16, ch // 16)].reshape(ch, 128).astype(F32).T
            for kx in range(3):
                f[kx, 2 - b // 3, 2 - b % 3] = t[kx * ch : (kx + 1) * ch]
    for r, (b, g) in enumerate(((b2, g2), (b1, g1))):
        b[...] = small[r : r + 1, :ch]
        g[...] = small[r : r + 1, ch : 2 * ch]


def per_device(volume, conv_one, conv_two, upper_grad, weight_one, weight_two,
               gain_one, bias_one, gain_two, bias_two):
    sizes = tuple(lax.axis_size(a) for a in AXES)
    n = math.prod(sizes)
    _, ch, nx, ny, nz = volume.shape
    cells = float(volume.shape[0] * nx * ny * nz * n)
    tiles = 9 * ch // 16
    per = -(-tiles // n)
    while tiles % per:
        per += 1

    vmem = pl.BlockSpec(memory_space=pltpu.VMEM)
    dma = pltpu.SemaphoreType.DMA
    big = pltpu.VMEM((nx, ny * ch, nz), F32)
    pad_u = pltpu.VMEM((ny, nx + 4, ch, nz), BF16)
    mid = pl.pallas_call(
        functools.partial(body, sizes, cells),
        name="section_backward",
        out_shape=(
            jax.ShapeDtypeStruct((nx, ny * ch, nz), BF16),
            jax.ShapeDtypeStruct((2, tiles, 16, 128), BF16),
            jax.ShapeDtypeStruct((8, 128), F32),
        ),
        in_specs=[vmem] * 10,
        out_specs=(vmem,) * 3,
        scratch_shapes=[
            big, big, big, big, pad_u, pad_u,
            pltpu.VMEM((2, nx + 2, ny + 2, 3, ch, nz), BF16),
            pltpu.VMEM((2, 9 * ch, 128), F32),
            pltpu.VMEM((2, tiles, 16, 128), BF16),
            pltpu.VMEM((3, n, 1, 128), F32),
            pltpu.VMEM((2, n, per, 16, 128), BF16),
            pltpu.VMEM((2, ch, -(-27 * ch // 128) * 128), BF16),
            pltpu.VMEM((4, nx + 2, ny + 2, ch, nz), BF16),
            pltpu.VMEM((2, 4, max(nx, ny) + 2, ch, nz), F32),
            pltpu.VMEM((4, max(nx, ny) + 2, ch, nz), F32),
            dma((3,)), dma((3,)), dma((4, 8)), dma((4, 8)),
            dma((2,)), dma((2,)), dma((2,)), dma((2,)),
        ],
        compiler_params=pltpu.CompilerParams(
            collective_id=0, has_side_effects=True, vmem_limit_bytes=60 * 1024 * 1024),
    )(conv_one[0], conv_two[0], upper_grad[0], volume[0], weight_one, weight_two,
      gain_one[None], bias_one[None], gain_two[None], bias_two[None])

    vector = jax.ShapeDtypeStruct((1, ch), F32)
    filt = jax.ShapeDtypeStruct(weight_one.shape, F32)
    out, *rest = pl.pallas_call(
        finish,
        name="section_finish",
        out_shape=(jax.ShapeDtypeStruct((ch, nx, ny, nz), BF16), filt, filt) + (vector,) * 4,
        in_specs=[vmem] * 3,
        out_specs=(vmem,) * 7,
    )(*mid)
    return (out[None], *rest[:2], *(v[0] for v in rest[2:]))


def solution(mesh):
    block = P("dp", None, "sx", "sy", None)
    return jax.shard_map(
        per_device,
        mesh=mesh,
        in_specs=(block,) * 4 + (P(),) * 6,
        out_specs=(block,) + (P(),) * 6,
        check_vma=False,
    )
```
